32 devices in a mesh: dp: 8 (over z, y), tensor: 4 (over x, core).
Axes of the slice: x: 2, y: 2, z: 4, core: 2. Of those that a mesh axis runs over, the one named last changes fastest.
Arguments:
- acts: bfloat16 [8192, 5120], P('dp', 'tensor'), may hold values from -6 to 6
- out_grad: bfloat16 [8192, 2048], P(('dp', 'tensor')), may hold values from -0.1875 to 0.1875
- momentum: float32 [40960, 2048], P(('dp', 'tensor')), may hold values from -100 to 100
- q_basis: float32 [2048, 256], P('tensor'), may hold values from -0.125 to 0.125
Outputs:
- new_momentum: float32 [40960, 2048], P(('dp', 'tensor'))
- ortho: float32 [5120, 256], P('tensor')
- new_q: float32 [2048, 256], P('tensor')
The draws below stay inside these ranges and needn't reach their ends.
All inputs are finite; a program needn't handle non-finite values.
Results may differ from the reference program's by a relative error of at most 0.0003.
Values may be sent and summed in bfloat16 or wider, within the bound.
No kernel may reach another device: no remote copies, remote signals or barrier semaphores. Data moves between devices by JAX's collectives and lax.ppermute only.
A program may use at most 64 MiB of HBM per device.

```python
import math
import jax
import jax.numpy as jnp
from jax import lax

D_IN = 5120
D_OUT = 2048
RANK = 256
TOK = 1024
TOKENS = 8192
N_DP = 8


def draw_momentum(key, part):
    key_base, key_rows, key_cols = jax.random.split(key, 3)
    base = jnp.clip(jax.random.normal(key_base, (N_DP * D_IN, D_OUT), jnp.float32), -6.0, 6.0)
    row_scale = jnp.exp(jax.random.uniform(key_rows, (N_DP * D_IN, 1), jnp.float32, math.log(0.5), math.log(2.0)))
    col_scale = jnp.exp(jax.random.uniform(key_cols, (1, D_OUT), jnp.float32, math.log(0.3), math.log(3.0)))
    return jnp.clip(base * row_scale * col_scale, -100.0, 100.0)


def block_scale(stream_key, dims, shards, low, largest):
    def one(dim, shards_of):
        draws = jax.random.uniform(jax.random.fold_in(jax.random.fold_in(stream_key, 6), dim), (shards_of,), jnp.float32, low / len(shards), largest / len(shards))
        return jnp.repeat(jnp.exp(draws), dims[dim] // shards_of).reshape((-1,) + (1,) * (len(dims) - dim - 1))

    factor_of = one(*shards[0])
    for cut in shards[1:]:
        factor_of = factor_of * one(*cut)
    return factor_of


def gaussian(rng, dims, scale, reach, cuts=(), held_as=jnp.bfloat16):
    level = block_scale(rng, dims, cuts, -0.22, 0.18) if cuts else 1.0
    drawn = jax.random.normal(rng, dims, jnp.float32) * scale * level
    return jnp.minimum(jnp.maximum(drawn, -reach), reach).astype(held_as)


def setup_inputs(seed: int = 0) -> dict:
    keys = jax.random.split(jax.random.key(seed), 5)
    return {
        "acts": gaussian(keys[0], (TOKENS, D_IN), 1.0, 6.0, ((0, 8), (1, 4))),
        "out_grad": gaussian(keys[1], (TOKENS, D_OUT), TOK ** -0.5, 0.1875, ((0, 32),)),
        "momentum": draw_momentum(jax.random.fold_in(keys[4], 71), 0),
        "q_basis": gaussian(keys[3], (D_OUT, RANK), D_OUT ** -0.5, 0.125, ((0, 4),), jnp.float32),
    }


def reference(acts, out_grad, momentum, q_basis):
    rows = acts.reshape(N_DP, TOK, D_IN)
    grads_out = out_grad.reshape(N_DP, TOK, D_OUT)
    moments = momentum.reshape(N_DP, D_IN, D_OUT)

    def make_buffer(index):
        grad = lax.dot_general(rows[index].astype(jnp.float32), grads_out[index].astype(jnp.float32), (((0,), (0,)), ((), ())), preferred_element_type=jnp.float32)
        return 0.95 * moments[index] + grad
    buffers = lax.map(make_buffer, jnp.arange(N_DP, dtype=jnp.int32))
    left = jnp.einsum('nij,jr->ir', buffers, q_basis, precision=lax.Precision.HIGHEST) / N_DP
    gram = jnp.dot(left.T, left, precision=lax.Precision.HIGHEST)
    chol = jnp.linalg.cholesky(gram)
    ortho = lax.linalg.triangular_solve(chol, left, left_side=False, lower=True, transpose_a=True)
    right = jnp.einsum('nij,ir->jr', buffers, ortho, precision=lax.Precision.HIGHEST) / N_DP
    update = jnp.dot(ortho, right.T, precision=lax.Precision.HIGHEST)
    new_momentum = (buffers - 0.05 * update[None]).reshape(N_DP * D_IN, D_OUT)
    new_q = right * lax.rsqrt(lax.optimization_barrier(jnp.sum(right * right, axis=0, keepdims=True)) + 1e-06)
    return (new_momentum, ortho, new_q)
```

```python
import functools

import jax
import jax.numpy as jnp
from jax import lax
from jax.experimental import pallas as pl
from jax.experimental.pallas import tpu as pltpu
from jax.sharding import PartitionSpec as P

F32 = jnp.float32
BF16 = jnp.bfloat16
HIGHEST = lax.Precision.HIGHEST
BLOCK = 32
GROUP = 8
LANES = 128


def split3(value):
    high = value.astype(BF16)
    rest = value - high.astype(F32)
    mid = rest.astype(BF16)
    low = (rest - mid.astype(F32)).astype(BF16)
    return high, mid, low


def chol_inverse_kernel(gram_ref, out_ref):
    n = gram_ref.shape[0]
    out_ref[...] = gram_ref[...]
    lane = lax.broadcasted_iota(jnp.int32, (GROUP, n), 1)
    sub = lax.broadcasted_iota(jnp.int32, (GROUP, LANES), 0)

    def wide(v):
        return jnp.concatenate([v] * (n // LANES), axis=1)

    groups = BLOCK // GROUP
    for block in range(n // BLOCK):
        base = block * BLOCK
        tile = [out_ref[pl.ds(base + g * GROUP, GROUP), :] for g in range(groups)]
        for g in range(groups):
            start = base + g * GROUP
            cols = [
                [
                    jnp.broadcast_to(tile[h][:, start + s : start + s + 1], (GROUP, LANES))
                    for h in range(g, groups)
                ]
                for s in range(GROUP)
            ]
            for s in range(GROUP):
                col = start + s
                scale = lax.rsqrt(jnp.broadcast_to(cols[s][0][s : s + 1, :], (GROUP, LANES)))
                factor = [c * scale for c in cols[s]]
                factor[0] = jnp.where(sub > s, factor[0], 0.0)
                pivot = jnp.broadcast_to(tile[g][s : s + 1, :], (GROUP, n)) * wide(scale)
                pivot = jnp.where(lane == col, wide(scale), pivot)
                for later in range(s + 1, GROUP):
                    entry = jnp.broadcast_to(cols[later][0][s : s + 1, :], (GROUP, LANES)) * scale
                    cols[later] = [c - f * entry for c, f in zip(cols[later], factor)]
                for h in range(g, groups):
                    if h == g:
                        kept = jnp.where((lane == col) & (wide(sub) > s), 0.0, tile[h])
                        new = kept - wide(factor[0]) * pivot
                        tile[h] = jnp.where(wide(sub) == s, pivot, new)
                    else:
                        kept = jnp.where(lane == col, 0.0, tile[h])
                        tile[h] = kept - wide(factor[h - g]) * pivot
        for g in range(groups):
            out_ref[pl.ds(base + g * GROUP, GROUP), :] = tile[g]
        rest = base + BLOCK
        if rest < n:
            rows = jnp.concatenate(tile, axis=0)
            lane_b = lax.broadcasted_iota(jnp.int32, (BLOCK, n), 1)
            row_b = lax.broadcasted_iota(jnp.int32, (BLOCK, n), 0) + base
            lower = jnp.where((lane_b > row_b) & (lane_b < rest), 0.0, rows)
            ah, am, al = split3(rows)
            bh, bm, bl = split3(lower)
            first = jnp.concatenate([ah, ah, ah, am, am, al], axis=0)
            second = jnp.concatenate([bh, bm, bl, bh, bm, bh], axis=0)
            change = lax.dot_general(
                first, second, (((0,), (0,)), ((), ())), preferred_element_type=F32
            )
            lane_r = lax.broadcasted_iota(jnp.int32, (n - rest, n), 1)
            old = out_ref[pl.ds(rest, n - rest), :]
            old = jnp.where((lane_r >= base) & (lane_r < rest), 0.0, old)
            out_ref[pl.ds(rest, n - rest), :] = old - change[rest:, :]
    lane_n = lax.broadcasted_iota(jnp.int32, (n, n), 1)
    row_n = lax.broadcasted_iota(jnp.int32, (n, n), 0)
    out_ref[...] = jnp.where(row_n >= lane_n, out_ref[...], 0.0)


def dot(a, b, contract, precision=None):
    return lax.dot_general(
        a, b, (contract, ((), ())), precision=precision, preferred_element_type=F32
    )


NN = ((1,), (0,))
NT = ((1,), (1,))
TN = ((0,), (0,))


def struct(shape, dtype=F32):
    return jax.ShapeDtypeStruct(shape, dtype)


def kernel_call(kernel, name, out, flops, *args, grid=(), in_specs=None, out_specs=None, scratch=()):
    whole = pl.BlockSpec(memory_space=pltpu.VMEM)
    many = isinstance(out, (tuple, list))
    if in_specs is None:
        in_specs = [None] * len(args)
    specs = []
    for spec, arg in zip(in_specs, args):
        if spec is None:
            spec = pl.BlockSpec(memory_space=pltpu.SMEM) if arg.dtype == jnp.int32 else whole
        specs.append(spec)
    if out_specs is None:
        out_specs = type(out)([whole] * len(out)) if many else whole
    moved = sum(a.size * a.dtype.itemsize for a in list(args) + list(out if many else [out]))
    return pl.pallas_call(
        kernel,
        out_shape=out,
        grid=grid,
        in_specs=specs,
        out_specs=out_specs,
        scratch_shapes=list(scratch),
        cost_estimate=pl.CostEstimate(flops=flops, bytes_accessed=moved, transcendentals=0),
        compiler_params=pltpu.CompilerParams(vmem_limit_bytes=34 * 1024 * 1024),
        name=name,
    )(*args)


def split2(value):
    high = value.astype(BF16)
    return high, (value - high.astype(F32)).astype(BF16)


def rows_at(index, rows):
    return pl.ds(pl.multiple_of(index * rows, rows), rows)


def chol_inverse(gram):
    n = gram.shape[0]
    return kernel_call(chol_inverse_kernel, "chol_inverse", struct((n, n)), 150_000_000, gram)


def basis_kernel(count, where_ref, grads_ref, *refs):
    pieces, (pair_ref, out_ref) = refs[:count], refs[count:]
    rows, rank = pieces[0].shape
    for m, piece in enumerate(pieces):
        high, low = split2(piece[...])
        at = rows_at(where_ref[0] ^ m, rows)
        pair_ref[at, :rank] = high
        pair_ref[at, rank:] = low
    both = dot(grads_ref[...], pair_ref[...], NN)
    out_ref[...] = both[:, :rank] + both[:, rank:]


def momentum_kernel(momentum_ref, pair_ref, out_ref):
    rank = out_ref.shape[1]
    high, low = split2(momentum_ref[...])
    both = dot(high, pair_ref[...], NN)
    out_ref[...] = 0.95 * (both[:, :rank] + both[:, rank:] + dot(low, pair_ref[:, :rank], NN))


def left_kernel(count, scale, where_ref, acts_ref, base_ref, *refs):
    pieces, (out_ref, pair_ref) = refs[:count], refs[count:]
    rows, rank = pieces[0].shape

    @pl.when(pl.program_id(0) == 0)
    def _():
        for m, piece in enumerate(pieces):
            high, low = split2(piece[...])
            at = rows_at(where_ref[0] ^ m, rows)
            pair_ref[at, :rank] = high
            pair_ref[at, rank:] = low

    both = dot(acts_ref[...], pair_ref[...], TN)
    out_ref[...] = scale * (base_ref[...] + (both[:, :rank] + both[:, rank:]))


def buffer_kernel(count, where_ref, acts_ref, momentum_ref, *refs):
    pieces, (high_ref, low_ref) = refs[:count], refs[count:]
    rows, columns = pieces[0].shape
    step = 512
    lhs = [acts_ref[rows_at(where_ref[0] ^ m, rows), :] for m in range(count)]
    for start in range(0, columns, step):
        at = slice(start, start + step)
        total = 0.95 * momentum_ref[:, at]
        for m in range(count):
            total = total + dot(lhs[m], pieces[m][:, at], TN)
        high_ref[:, at], low_ref[:, at] = split2(total)


def gram_kernel(*refs):
    pieces, out_ref = refs[:-1], refs[-1]
    total = None
    for piece in pieces:
        value = piece[...]
        term = dot(value, value, TN, HIGHEST)
        total = term if total is None else total + term
    out_ref[...] = total


def share_kernel(count, scale, where_ref, high_ref, low_ref, *refs):
    pieces, (out_ref, pair_ref) = refs[:count], refs[count:]
    rows, rank = pieces[0].shape

    @pl.when(pl.program_id(0) == 0)
    def _():
        for m, piece in enumerate(pieces):
            high, low = split2(piece[...] * scale)
            at = rows_at(where_ref[1] ^ m, rows)
            pair_ref[at, :rank] = high
            pair_ref[at, rank:] = low

    both = dot(pair_ref[...], high_ref[...], TN)
    total = both[:rank] + both[rank:] + dot(pair_ref[:, :rank], low_ref[...], TN)
    out_ref[...] = total.T


def right_kernel(part_ref, inverse_ref, right_ref, narrow_ref):
    right = dot(part_ref[...], inverse_ref[...], NT, HIGHEST)
    right_ref[...] = right
    narrow_ref[...] = right.astype(BF16)


def ortho_kernel(count, where_ref, inverse_ref, *refs):
    pieces, out_ref = refs[:count], refs[count]
    rows = pieces[0].shape[0]
    for m, piece in enumerate(pieces):
        out_ref[rows_at(where_ref[1] ^ m, rows), :] = dot(piece[...], inverse_ref[...], NT, HIGHEST)


def collect_kernel(xs, quad, where_ref, *refs):
    exact, narrow = refs[:quad], refs[quad : quad + (xs - 1) * quad]
    own_ref, side_ref, squares_ref = refs[-3:]
    rows = exact[0].shape[0]
    squares = None
    for m in range(quad):
        value = exact[m][...]
        at = rows_at(where_ref[1] ^ m, rows)
        own_ref[at, :] = value
        side_ref[0, at, :] = value.astype(BF16)
        term = jnp.sum(value * value, axis=0, keepdims=True)
        squares = term if squares is None else squares + term
        for x in range(1, xs):
            side_ref[x, at, :] = narrow[(x - 1) * quad + m][...]
    squares_ref[...] = jnp.broadcast_to(squares, squares_ref.shape)


def update_kernel(xs, where_ref, high_ref, low_ref, ortho_ref, side_ref, other_ref, out_ref, full_ref):
    rows = side_ref.shape[1]
    columns = out_ref.shape[1]

    @pl.when(pl.program_id(0) == 0)
    def _():
        for x in range(xs):
            full_ref[rows_at(where_ref[0] ^ (2 * x), rows), :] = side_ref[x]
            full_ref[rows_at(where_ref[0] ^ (2 * x + 1), rows), :] = other_ref[x]

    ortho = ortho_ref[...].astype(BF16)
    step = 512
    for start in range(0, columns, step):
        at = slice(start, start + step)
        change = dot(ortho, full_ref[at, :], NT)
        value = high_ref[:, at].astype(F32) + low_ref[:, at].astype(F32)
        out_ref[:, at] = value - 0.05 * change


class Exchange:
    def __init__(self, replicas, parts):
        self.replicas, self.parts = replicas, parts
        self.quad = min(4, replicas)
        self.xs = parts // 2
        self.higher = []
        bit = self.quad
        while bit < replicas:
            self.higher.append(bit | (bit >> 1))
            bit *= 2
        d, self.t = lax.axis_index("dp"), lax.axis_index("tensor")
        bits, k, above = [], replicas.bit_length() - 2, 0
        while k >= 0:
            own = (d >> k) & 1
            if k >= 1 and (1 << (k + 1)) < replicas:
                own = own ^ above
            bits.append((k, own))
            above = own
            k -= 1
        self.q = sum(own << k for k, own in bits if (1 << k) < self.quad)
        self.x, self.core = self.t // 2, self.t % 2

    def swap(self, value, dp=0, tensor=0):
        n, m = self.parts, self.replicas
        if dp == 0:
            return lax.ppermute(value, "tensor", [(i, i ^ tensor) for i in range(n)])
        if tensor == 0:
            return lax.ppermute(value, "dp", [(i, i ^ dp) for i in range(m)])
        pairs = [((i // n), i % n) for i in range(m * n)]
        perm = [(d * n + t, (d ^ dp) * n + (t ^ tensor)) for d, t in pairs]
        return lax.ppermute(value, ("dp", "tensor"), perm)

    def gather_tensor(self, value):
        pieces = {0: value, 1: self.swap(value, tensor=1)}
        for m in range(2, self.parts, 2):
            pieces[m] = self.swap(value, tensor=m)
            pieces[m + 1] = self.swap(pieces[m], tensor=1)
        return [pieces[m] for m in range(self.parts)]


def block(value, index, count):
    rows = value.shape[0] // count
    return lax.dynamic_slice_in_dim(value, index * rows, rows, axis=0)


def body(acts, out_grad, momentum, q_basis):
    replicas, parts = lax.axis_size("dp"), lax.axis_size("tensor")
    ex = Exchange(replicas, parts)
    rows, columns = momentum.shape
    tokens = acts.shape[0]
    rank = q_basis.shape[1]
    tile = 256 if rows % 256 == 0 else 128
    steps = rows // tile
    where = jnp.stack([ex.t, ex.q]).astype(jnp.int32)
    wide_spec = pl.BlockSpec((tile, columns), lambda i: (i, 0))
    rank_spec = pl.BlockSpec((tile, rank), lambda i: (i, 0))
    acts_spec = pl.BlockSpec((tokens, tile), lambda i: (0, i))

    basis = ex.gather_tensor(q_basis)
    pair, grad_q = kernel_call(
        functools.partial(basis_kernel, parts), "basis",
        (struct((columns, 2 * rank), BF16), struct((out_grad.shape[0], rank))),
        4 * out_grad.shape[0] * columns * rank, where, out_grad, *basis,
    )
    grads_q = ex.gather_tensor(grad_q)
    base = kernel_call(
        momentum_kernel, "momentum_q", struct((rows, rank)), 6 * rows * columns * rank,
        momentum, pair, grid=(steps,), in_specs=[wide_spec, None], out_specs=rank_spec,
    )
    left = kernel_call(
        functools.partial(left_kernel, parts, 1.0 / replicas), "left", struct((rows, rank)),
        4 * rows * tokens * rank, where, acts, base, *grads_q, grid=(steps,),
        in_specs=[None, acts_spec, rank_spec] + [None] * parts, out_specs=rank_spec,
        scratch=[pltpu.VMEM((tokens, 2 * rank), BF16)],
    )

    held, _ = lax.optimization_barrier((out_grad, grads_q[2 % parts]))
    grads = ex.gather_tensor(held)
    high, low = kernel_call(
        functools.partial(buffer_kernel, parts), "buffer",
        (struct((rows, columns), BF16), struct((rows, columns), BF16)),
        2 * rows * tokens * columns, where, acts, momentum, *grads, grid=(steps,),
        in_specs=[None, acts_spec, wide_spec] + [None] * parts, out_specs=(wide_spec, wide_spec),
    )

    quad = range(1, ex.quad)
    part = block(left, ex.q, ex.quad)
    for piece in [ex.swap(block(left, ex.q ^ m, ex.quad), dp=m) for m in quad]:
        part = part + piece
    for mask in ex.higher:
        part = part + ex.swap(part, dp=mask)
    lefts = [part] + [ex.swap(part, dp=m) for m in quad]

    gram = kernel_call(gram_kernel, "gram", struct((rank, rank)), 12 * rows * rank * rank, *lefts)
    gram = gram + ex.swap(gram, tensor=1)
    total = gram
    for m in range(1, ex.xs):
        total = total + ex.swap(gram, tensor=2 * m)
    inverse = chol_inverse(total)

    step = 512
    half_spec = pl.BlockSpec((rows, step), lambda i: (0, i))
    share = kernel_call(
        functools.partial(share_kernel, ex.quad, 1.0 / replicas), "share", struct((columns, rank)),
        6 * rows * columns * rank, where, high, low, *lefts, grid=(columns // step,),
        in_specs=[None, half_spec, half_spec] + [None] * ex.quad,
        out_specs=pl.BlockSpec((step, rank), lambda i: (i, 0)),
        scratch=[pltpu.VMEM((rows, 2 * rank), BF16)],
    )
    share = share.reshape(ex.xs, 2, -1, rank)
    keep = lax.dynamic_index_in_dim(share, ex.core, 1, keepdims=False)
    send = lax.dynamic_index_in_dim(share, 1 - ex.core, 1, keepdims=False)
    share = (keep + ex.swap(send, tensor=1)).reshape(-1, rank)
    count = ex.xs * ex.quad
    mine = ex.x * ex.quad + ex.q
    part = block(share, mine, count)
    for piece in [
        ex.swap(block(share, mine ^ m, count), dp=m % ex.quad, tensor=2 * (m // ex.quad))
        for m in range(1, count)
    ]:
        part = part + piece
    for mask in ex.higher:
        part = part + ex.swap(part, dp=mask)

    right, narrow = kernel_call(
        right_kernel, "right", (struct(part.shape), struct(part.shape, BF16)),
        12 * part.shape[0] * rank * rank, part, inverse,
    )
    exact = [right] + [ex.swap(right, dp=m) for m in quad]
    across = [
        ex.swap(narrow, dp=m % ex.quad, tensor=2 * (m // ex.quad)) for m in range(ex.quad, count)
    ]
    local = columns // parts
    own, side, squares = kernel_call(
        functools.partial(collect_kernel, ex.xs, ex.quad), "collect",
        (struct((local, rank)), struct((ex.xs, local, rank), BF16), struct((8, rank))),
        2 * local * rank, where, *exact, *across,
    )
    other = ex.swap(side, tensor=1)
    squares = squares + ex.swap(squares, tensor=1)
    col_squares = squares
    for m in range(1, ex.xs):
        col_squares = col_squares + ex.swap(squares, tensor=2 * m)
    new_q = own * lax.rsqrt(col_squares[:1] + 1e-06)

    ortho = kernel_call(
        functools.partial(ortho_kernel, ex.quad), "ortho", struct((rows, rank)),
        12 * rows * rank * rank, where, inverse, *lefts,
    )
    new_momentum = kernel_call(
        functools.partial(update_kernel, ex.xs), "update", struct((rows, columns)),
        2 * rows * columns * rank, where, high, low, ortho, side, other, grid=(steps,),
        in_specs=[None, wide_spec, wide_spec, rank_spec, None, None], out_specs=wide_spec,
        scratch=[pltpu.VMEM((columns, rank), BF16)],
    )
    return (new_momentum, ortho, new_q)


def solution(mesh):
    in_specs = (
        P("dp", "tensor"),
        P(("dp", "tensor"), None),
        P(("dp", "tensor"), None),
        P("tensor", None),
    )
    out_specs = (P(("dp", "tensor"), None), P("tensor", None), P("tensor", None))
    return jax.shard_map(body, mesh=mesh, in_specs=in_specs, out_specs=out_specs, check_vma=False)
```

```python
import functools

import jax
import jax.numpy as jnp
from jax import lax
from jax.experimental import pallas as pl
from jax.experimental.pallas import tpu as pltpu
from jax.sharding import PartitionSpec as P


F32 = jnp.float32
BF16 = jnp.bfloat16
HIGHEST = lax.Precision.HIGHEST
BLOCK = 32
GROUP = 8
VMEM = 20
LARGE = 54
LEFT = 60
LANES = 128


def split3(value):
    high = value.astype(BF16)
    rest = value - high.astype(F32)
    mid = rest.astype(BF16)
    low = (rest - mid.astype(F32)).astype(BF16)
    return high, mid, low


def chol_inverse_kernel(first, last, gram_ref, out_ref):
    n = gram_ref.shape[0]
    out_ref[...] = gram_ref[...]
    lane = lax.broadcasted_iota(jnp.int32, (GROUP, n), 1)
    sub = lax.broadcasted_iota(jnp.int32, (GROUP, LANES), 0)

    def wide(v):
        return jnp.concatenate([v] * (n // LANES), axis=1)

    groups = BLOCK // GROUP
    for block in range(first, last):
        base = block * BLOCK
        tile = [out_ref[pl.ds(base + g * GROUP, GROUP), :] for g in range(groups)]
        for g in range(groups):
            start = base + g * GROUP
            cols = [
                [
                    jnp.broadcast_to(tile[h][:, start + s : start + s + 1], (GROUP, LANES))
                    for h in range(g, groups)
                ]
                for s in range(GROUP)
            ]
            for s in range(GROUP):
                col = start + s
                scale = lax.rsqrt(jnp.broadcast_to(cols[s][0][s : s + 1, :], (GROUP, LANES)))
                factor = [c * scale for c in cols[s]]
                factor[0] = jnp.where(sub > s, factor[0], 0.0)
                pivot = jnp.broadcast_to(tile[g][s : s + 1, :], (GROUP, n)) * wide(scale)
                pivot = jnp.where(lane == col, wide(scale), pivot)
                for later in range(s + 1, GROUP):
                    entry = jnp.broadcast_to(cols[later][0][s : s + 1, :], (GROUP, LANES)) * scale
                    cols[later] = [c - f * entry for c, f in zip(cols[later], factor)]
                for h in range(g, groups):
                    if h == g:
                        kept = jnp.where((lane == col) & (wide(sub) > s), 0.0, tile[h])
                        new = kept - wide(factor[0]) * pivot
                        tile[h] = jnp.where(wide(sub) == s, pivot, new)
                    else:
                        kept = jnp.where(lane == col, 0.0, tile[h])
                        tile[h] = kept - wide(factor[h - g]) * pivot
        for g in range(groups):
            out_ref[pl.ds(base + g * GROUP, GROUP), :] = tile[g]
        rest = base + BLOCK
        if rest < n:
            rows = jnp.concatenate(tile, axis=0)
            lane_b = lax.broadcasted_iota(jnp.int32, (BLOCK, n), 1)
            row_b = lax.broadcasted_iota(jnp.int32, (BLOCK, n), 0) + base
            lower = jnp.where((lane_b > row_b) & (lane_b < rest), 0.0, rows)
            ah, am, al = split3(rows)
            bh, bm, bl = split3(lower)
            first = jnp.concatenate([ah, ah, ah, am, am, al], axis=0)
            second = jnp.concatenate([bh, bm, bl, bh, bm, bh], axis=0)
            change = lax.dot_general(
                first, second, (((0,), (0,)), ((), ())), preferred_element_type=F32
            )
            lane_r = lax.broadcasted_iota(jnp.int32, (n - rest, n), 1)
            old = out_ref[pl.ds(rest, n - rest), :]
            old = jnp.where((lane_r >= base) & (lane_r < rest), 0.0, old)
            out_ref[pl.ds(rest, n - rest), :] = old - change[rest:, :]
    if last * BLOCK == n:
        lane_n = lax.broadcasted_iota(jnp.int32, (n, n), 1)
        row_n = lax.broadcasted_iota(jnp.int32, (n, n), 0)
        out_ref[...] = jnp.where(row_n >= lane_n, out_ref[...], 0.0)


def dot(a, b, contract, precision=None):
    return lax.dot_general(
        a, b, (contract, ((), ())), precision=precision, preferred_element_type=F32
    )


NN = ((1,), (0,))
NT = ((1,), (1,))
TN = ((0,), (0,))


def struct(shape, dtype=F32):
    return jax.ShapeDtypeStruct(shape, dtype)


def kernel_call(kernel, out, flops, *args, grid=(), in_specs=None, out_specs=None, scratch=(), vmem=VMEM, prefetch=0):
    whole = pl.BlockSpec(memory_space=pltpu.VMEM)
    many = isinstance(out, (tuple, list))
    if in_specs is None:
        in_specs = [None] * len(args)
    specs = []
    for i, (spec, arg) in enumerate(zip(in_specs, args)):
        if i < prefetch:
            continue
        if spec is None:
            spec = pl.BlockSpec(memory_space=pltpu.SMEM) if arg.dtype == jnp.int32 else whole
        specs.append(spec)
    if out_specs is None:
        out_specs = type(out)([whole] * len(out)) if many else whole
    moved = sum(a.size * a.dtype.itemsize for a in list(args) + list(out if many else [out]))
    return pl.pallas_call(
        kernel,
        out_shape=out,
        grid_spec=pltpu.PrefetchScalarGridSpec(
            num_scalar_prefetch=prefetch,
            grid=grid,
            in_specs=specs,
            out_specs=out_specs,
            scratch_shapes=list(scratch),
        ),
        cost_estimate=pl.CostEstimate(flops=flops, bytes_accessed=moved, transcendentals=0),
        compiler_params=pltpu.CompilerParams(vmem_limit_bytes=vmem * 1024 * 1024),
    )(*args)


def split2(value):
    high = value.astype(BF16)
    return high, (value - high.astype(F32)).astype(BF16)


def rows_at(index, rows):
    return pl.ds(pl.multiple_of(index * rows, rows), rows)


def chol_inverse(state, first, last):
    kernel = functools.partial(chol_inverse_kernel, first, last)
    return kernel_call(kernel, struct(state.shape), 2_000_000_000, state)


def tied(values, *others):
    return lax.optimization_barrier((values, others))[0]


def fill_pair(pair_ref, pieces, place, scale=1.0):
    rows, rank = pieces[0].shape
    for m, piece in enumerate(pieces):
        high, low = split2(piece[...] * scale if scale != 1.0 else piece[...])
        at = rows_at(place(m), rows)
        pair_ref[at, :rank] = high
        pair_ref[at, rank:] = low


def basis_kernel(first, count, where_ref, grads_ref, *refs):
    pieces, (pair_ref, out_ref) = refs[: 2 * count], refs[-2:]
    rows, rank = pieces[0].shape
    fill_pair(pair_ref, pieces, lambda m: (m // 2) * 2 + ((where_ref[0] ^ m) & 1))
    total = refs[2 * count][...] if first else None
    for m in range(count):
        block = (where_ref[0] >> 1) ^ (first + m)
        columns = pl.ds(pl.multiple_of(block * (2 * rows), 2 * rows), 2 * rows)
        both = dot(grads_ref[:, columns], pair_ref[m * 2 * rows : (m + 1) * 2 * rows, :], NN)
        term = both[:, :rank] + both[:, rank:]
        total = term if total is None else total + term
    out_ref[...] = total


def momentum_kernel(first, where_ref, momentum_ref, pair_ref, *refs):
    out_ref = refs[-1]
    rank = out_ref.shape[1]
    high, low = split2(momentum_ref[...])
    both = dot(high, pair_ref[...], NN)
    term = 0.95 * (both[:, :rank] + both[:, rank:] + dot(low, pair_ref[:, :rank], NN))

    if first == 0:
        out_ref[...] = term
        return

    @pl.when(pl.program_id(1) == 0)
    def _():
        out_ref[...] = refs[0][...] + term

    @pl.when(pl.program_id(1) != 0)
    def _():
        out_ref[...] = out_ref[...] + term


SPLIT = 2


def chunk_of(q, index):
    return (q ^ (index // SPLIT)) * SPLIT + index % SPLIT


def left_kernel(count, scale, where_ref, acts_ref, base_ref, *refs):
    pieces, outs, (pair_ref, full_ref) = refs[:count], refs[count:-2], refs[-2:]
    rank = pieces[0].shape[1]
    fill_pair(pair_ref, pieces, lambda m: where_ref[0] ^ m)
    both = dot(acts_ref[...], pair_ref[...], TN)
    full_ref[...] = scale * (base_ref[...] + (both[:, :rank] + both[:, rank:]))
    for m, out_ref in enumerate(outs):
        out_ref[...] = full_ref[rows_at(chunk_of(where_ref[1], m), out_ref.shape[0]), :]


def buffer_kernel(count, where_ref, acts_ref, momentum_ref, *refs):
    pieces, (high_ref, low_ref) = refs[:count], refs[count:]
    rows, columns = pieces[0].shape
    step = 512
    lhs = [acts_ref[rows_at(where_ref[0] ^ m, rows), :] for m in range(count)]
    for start in range(0, columns, step):
        at = slice(start, start + step)
        total = 0.95 * momentum_ref[:, at]
        for m in range(count):
            total = total + dot(lhs[m], pieces[m][:, at], TN)
        high_ref[:, at], low_ref[:, at] = split2(total)


def gram_kernel(*refs):
    pieces, out_ref = refs[:-1], refs[-1]
    total = None
    for piece in pieces:
        value = piece[...]
        term = dot(value, value, TN, HIGHEST)
        total = term if total is None else total + term
    out_ref[...] = total


def share_kernel(quad, scale, where_ref, high_ref, low_ref, *refs):
    pieces, (out_ref, pair_ref) = refs[:-2], refs[-2:]
    rank = pieces[0].shape[1]

    @pl.when((pl.program_id(0) == 0) & (pl.program_id(1) == 0))
    def _():
        fill_pair(pair_ref, pieces, lambda m: chunk_of(where_ref[1], m), scale)

    both = dot(pair_ref[...], high_ref[...], TN)
    total = both[:rank] + both[rank:] + dot(pair_ref[:, :rank], low_ref[...], TN)
    total = total.T
    chunk = total.shape[0] // quad
    for c in range(quad):
        out_ref[0, 0, rows_at(where_ref[1] ^ c, chunk), :] = total[c * chunk : (c + 1) * chunk]


EXTRA = 16


def with_squares(ref, start, squares):
    ref[start : start + EXTRA, :] = jnp.zeros((EXTRA, ref.shape[1]), BF16)
    for i, part in enumerate(split3(squares)):
        ref[start + i : start + i + 1, :] = part


def squares_of(ref, start):
    part = ref[start : start + EXTRA, :].astype(F32)
    return part[0:1] + part[1:2] + part[2:3]


def right_kernel(part_ref, inverse_ref, right_ref, narrow_ref):
    right = dot(part_ref[...], inverse_ref[...], NT, HIGHEST)
    rows = right.shape[0]
    right_ref[...] = right
    narrow_ref[:rows, :] = right.astype(BF16)
    with_squares(narrow_ref, rows, jnp.sum(right * right, axis=0, keepdims=True))


def ortho_kernel(where_ref, inverse_ref, *refs):
    pieces, (out_ref, narrow_ref) = refs[:-2], refs[-2:]
    rows = pieces[0].shape[0]
    for m, piece in enumerate(pieces):
        at = rows_at(chunk_of(where_ref[1], m), rows)
        value = dot(piece[...], inverse_ref[...], NT, HIGHEST)
        out_ref[at, :] = value
        narrow_ref[at, :] = value.astype(BF16)


def collect_kernel(xs, quad, where_ref, *refs):
    exact, narrow = refs[:quad], refs[quad : xs * quad]
    own_ref, side_ref = refs[-2:]
    rows = exact[0].shape[0]
    squares = None
    for m in range(quad):
        value = exact[m][...]
        own_ref[rows_at(where_ref[1] ^ m, rows), :] = value
        terms = [jnp.sum(value * value, axis=0, keepdims=True)]
        for x in range(xs):
            at = rows_at(x * quad + (where_ref[1] ^ m), rows)
            if x == 0:
                side_ref[at, :] = value.astype(BF16)
            else:
                piece = narrow[(x - 1) * quad + m]
                side_ref[at, :] = piece[:rows, :]
                terms.append(squares_of(piece, rows))
        for term in terms:
            squares = term if squares is None else squares + term
    with_squares(side_ref, xs * quad * rows, squares)


def update_kernel(xs, where_ref, high_ref, low_ref, ortho_ref, side_ref, other_ref, own_ref, out_ref, new_ref, full_ref):
    rows = own_ref.shape[0]

    @pl.when(pl.program_id(0) == 0)
    def _():
        for x in range(xs):
            at = slice(x * rows, (x + 1) * rows)
            full_ref[rows_at(where_ref[0] ^ (2 * x), rows), :] = side_ref[at, :]
            full_ref[rows_at(where_ref[0] ^ (2 * x + 1), rows), :] = other_ref[at, :]
        squares = squares_of(side_ref, xs * rows) + squares_of(other_ref, xs * rows)
        new_ref[...] = own_ref[...] * lax.rsqrt(squares + 1e-06)

    step = 512
    for start in range(0, out_ref.shape[1], step):
        at = slice(start, start + step)
        change = dot(ortho_ref[...], full_ref[at, :], NT)
        value = high_ref[:, at].astype(F32) + low_ref[:, at].astype(F32)
        out_ref[:, at] = value - 0.05 * change


class Exchange:
    def __init__(self, replicas, parts):
        self.replicas, self.parts = replicas, parts
        self.quad = min(4, replicas)
        self.xs = parts // 2
        self.higher = []
        bit = self.quad
        while bit < replicas:
            self.higher.append(bit | (bit >> 1))
            bit *= 2
        d, self.t = lax.axis_index("dp"), lax.axis_index("tensor")
        bits, k, above = [], replicas.bit_length() - 2, 0
        while k >= 0:
            own = (d >> k) & 1
            if k >= 1 and (1 << (k + 1)) < replicas:
                own = own ^ above
            bits.append((k, own))
            above = own
            k -= 1
        self.q = sum(own << k for k, own in bits if (1 << k) < self.quad)
        self.x, self.core = self.t // 2, self.t % 2

    def swap(self, value, dp=0, tensor=0):
        n, m = self.parts, self.replicas
        if dp == 0:
            return lax.ppermute(value, "tensor", [(i, i ^ tensor) for i in range(n)])
        if tensor == 0:
            return lax.ppermute(value, "dp", [(i, i ^ dp) for i in range(m)])
        pairs = [((i // n), i % n) for i in range(m * n)]
        perm = [(d * n + t, (d ^ dp) * n + (t ^ tensor)) for d, t in pairs]
        return lax.ppermute(value, ("dp", "tensor"), perm)

    def gather_tensor(self, value):
        pieces = {0: value, 1: self.swap(value, tensor=1)}
        for m in range(2, self.parts, 2):
            pieces[m] = self.swap(value, tensor=m)
            pieces[m + 1] = self.swap(pieces[m], tensor=1)
        return [pieces[m] for m in range(self.parts)]


def step(acts, out_grad, momentum, q_basis):
    replicas, parts = lax.axis_size("dp"), lax.axis_size("tensor")
    ex = Exchange(replicas, parts)
    rows, columns = momentum.shape
    tokens = acts.shape[0]
    rank = q_basis.shape[1]
    tile = 256 if rows % 256 == 0 else 128
    large = rows // 2
    steps = rows // tile
    where = jnp.stack([ex.t, ex.q]).astype(jnp.int32)
    wide_spec = pl.BlockSpec((tile, columns), lambda i: (i, 0))
    rank_spec = pl.BlockSpec((tile, rank), lambda i: (i, 0))
    acts_spec = pl.BlockSpec((tokens, tile), lambda i: (0, i))

    xs, local = ex.xs, columns // parts
    half = 2 * local
    where_x = jnp.stack([ex.x, ex.q]).astype(jnp.int32)
    near = [q_basis, ex.swap(q_basis, tensor=1)]
    across = [ex.swap(q_basis, tensor=m) for m in range(2, parts, 2)]

    def basis(first, pieces, *more):
        count = len(pieces) // 2
        return kernel_call(
            functools.partial(basis_kernel, first, count),
            (struct((count * half, 2 * rank), BF16), struct((out_grad.shape[0], rank))),
            4 * out_grad.shape[0] * count * half * rank, where, out_grad, *pieces, *more,
        )

    near_pair, near_grad = basis(0, near)
    base = kernel_call(
        functools.partial(momentum_kernel, 0), struct((rows, rank)),
        6 * rows * half * rank, where_x, momentum, near_pair, grid=(2,), prefetch=1,
        in_specs=[None, pl.BlockSpec((large, half), lambda i, w: (i, w[0])), None],
        out_specs=pl.BlockSpec((large, rank), lambda i, w: (i, 0)), vmem=LARGE,
    )
    far = []
    for piece in tied(across, base):
        far += [piece, ex.swap(piece, tensor=1)]
    pair, grad_q = basis(1, far, near_grad)
    base = kernel_call(
        functools.partial(momentum_kernel, 1), struct((rows, rank)),
        6 * rows * (columns - half) * rank, where_x, momentum, pair, base,
        grid=(2, xs - 1), prefetch=1,
        in_specs=[
            None,
            pl.BlockSpec((large, half), lambda i, j, w: (i, w[0] ^ (j + 1))),
            pl.BlockSpec((half, 2 * rank), lambda i, j, w: (j, 0)),
            pl.BlockSpec((large, rank), lambda i, j, w: (i, 0)),
        ],
        out_specs=pl.BlockSpec((large, rank), lambda i, j, w: (i, 0)), vmem=LARGE,
    )
    near_q = ex.swap(grad_q, tensor=1)
    far_q = tied([ex.swap(grad_q, tensor=m) for m in range(2, parts, 2)], base)
    grads_q = [grad_q, near_q]
    for value in far_q:
        grads_q += [value, ex.swap(value, tensor=1)]
    left = kernel_call(
        functools.partial(left_kernel, parts, 1.0 / replicas),
        [struct((rows // (SPLIT * ex.quad), rank))] * (SPLIT * ex.quad),
        4 * rows * tokens * rank, where, acts, base, *grads_q,
        scratch=[pltpu.VMEM((tokens, 2 * rank), BF16), pltpu.VMEM((rows, rank), F32)], vmem=LEFT,
    )

    quad = range(1, ex.quad)
    received = []
    for h in range(SPLIT):
        received.append([ex.swap(left[m * SPLIT + h], dp=m) for m in quad])
    grads = {0: out_grad, 1: ex.swap(out_grad, tensor=1)}
    sums = []
    for h in range(SPLIT):
        total = left[h]
        for piece in tied(received[h], sums):
            total = total + piece
        sums.append(total)
    held = tied(out_grad, grads_q[1:])
    for m in range(2, parts, 2):
        grads[m] = ex.swap(held, tensor=m)
    for mask in ex.higher:
        others = [ex.swap(value, dp=mask) for value in sums]
        added = []
        for value, other in zip(sums, others):
            added.append(value + tied(other, added))
        sums = added
    for m in range(2, parts, 2):
        grads[m] = tied(grads[m], sums)
        grads[m + 1] = ex.swap(grads[m], tensor=1)
    lefts = list(sums)
    for m in quad:
        lefts += [ex.swap(value, dp=m) for value in sums]
    grads = [grads[m] for m in range(parts)]

    high, low = kernel_call(
        functools.partial(buffer_kernel, parts),
        (struct((rows, columns), BF16), struct((rows, columns), BF16)),
        2 * rows * tokens * columns, where, acts, momentum, *grads, grid=(steps,),
        in_specs=[None, acts_spec, wide_spec] + [None] * parts, out_specs=(wide_spec, wide_spec), vmem=34,
    )

    lefts[SPLIT:] = tied(lefts[SPLIT:], high)
    gram = kernel_call(gram_kernel, struct((rank, rank)), 12 * rows * rank * rank, *lefts)
    lefts_b = tied(lefts, gram)
    near_gram = ex.swap(gram, tensor=1)
    blocks = rank // BLOCK
    count = xs * ex.quad

    def shares(other, first, number):
        core = 1 - ex.core if other else ex.core
        at = jnp.stack([ex.x * 2 + core, ex.q, core]).astype(jnp.int32)
        spec = pl.BlockSpec((rows, local), lambda i, j, w: (0, w[0] ^ (2 * (i + first))))
        return kernel_call(
            functools.partial(share_kernel, ex.quad, 1.0 / replicas),
            struct((number, 1, local, rank)), 6 * rows * number * local * rank,
            at, high, low, *lefts_b, grid=(number, 1), prefetch=1,
            in_specs=[None, spec, spec] + [None] * len(lefts_b),
            out_specs=pl.BlockSpec((1, 1, local, rank), lambda i, j, w: (i, 0, 0, 0)),
            scratch=[pltpu.VMEM((rows, 2 * rank), BF16)], vmem=VMEM,
        ).reshape(number * ex.quad, local // ex.quad, rank)

    send = shares(True, 0, xs)
    got = ex.swap(send, tensor=1)
    gram = gram + tied(near_gram, send)
    grams = [ex.swap(gram, tensor=m) for m in range(2, parts, 2)]
    keep = shares(False, 0, xs)
    share = keep + got
    part = share[0]
    pieces = [
        ex.swap(share[m], dp=m % ex.quad, tensor=2 * (m // ex.quad)) for m in range(1, count)
    ]
    total = gram
    for piece in tied(grams, pieces[-1]):
        total = total + piece
    state = chol_inverse(total, 0, blocks // 2)
    for piece in tied(pieces, state):
        part = part + piece
    inverse = chol_inverse(tied(state, part), blocks // 2, blocks)
    for mask in ex.higher:
        part = part + tied(ex.swap(part, dp=mask), inverse)

    right, narrow = kernel_call(
        right_kernel, (struct(part.shape), struct((part.shape[0] + EXTRA, rank), BF16)),
        12 * part.shape[0] * rank * rank, part, inverse,
    )
    exact = [right] + [ex.swap(right, dp=m) for m in quad]
    across = [
        ex.swap(narrow, dp=m % ex.quad, tensor=2 * (m // ex.quad)) for m in range(ex.quad, count)
    ]
    ortho, narrow = kernel_call(
        ortho_kernel,
        (struct((rows, rank)), struct((rows, rank), BF16)),
        12 * rows * rank * rank, tied(where, right), inverse, *lefts,
    )
    exact[1:], across = tied((exact[1:], across), ortho)
    own, side = kernel_call(
        functools.partial(collect_kernel, xs, ex.quad),
        (struct((local, rank)), struct((xs * local + EXTRA, rank), BF16)),
        2 * local * rank, where, *exact, *across,
    )
    other = ex.swap(side, tensor=1)
    new_momentum, new_q = kernel_call(
        functools.partial(update_kernel, xs),
        (struct((rows, columns)), struct((local, rank))),
        2 * rows * columns * rank, where, high, low, narrow, side, other, own, grid=(steps,),
        in_specs=[None, wide_spec, wide_spec, rank_spec, None, None, None],
        out_specs=(wide_spec, pl.BlockSpec((local, rank), lambda i: (0, 0))),
        scratch=[pltpu.VMEM((columns, rank), BF16)], vmem=VMEM,
    )
    return (new_momentum, ortho, new_q)


def solution(mesh):
    in_specs = (
        P("dp", "tensor"),
        P(("dp", "tensor"), None),
        P(("dp", "tensor"), None),
        P("tensor", None),
    )
    out_specs = (P(("dp", "tensor"), None), P("tensor", None), P("tensor", None))
    return jax.shard_map(step, mesh=mesh, in_specs=in_specs, out_specs=out_specs, check_vma=False)
```

```python
import functools

import jax
import jax.numpy as jnp
from jax import lax
from jax.experimental import pallas as pl
from jax.experimental.pallas import tpu as pltpu
from jax.sharding import PartitionSpec as P


F32 = jnp.float32
BF16 = jnp.bfloat16
HIGHEST = lax.Precision.HIGHEST
BLOCK = 32
GROUP = 8
VMEM = 20
LARGE = 52
LEFT = 60
BUFFER = 34
LANES = 128


def split3(value):
    high = value.astype(BF16)
    rest = value - high.astype(F32)
    mid = rest.astype(BF16)
    low = (rest - mid.astype(F32)).astype(BF16)
    return high, mid, low


def chol_inverse_kernel(first, last, gram_ref, out_ref):
    n = gram_ref.shape[0]
    out_ref[...] = gram_ref[...]
    lane = lax.broadcasted_iota(jnp.int32, (GROUP, n), 1)
    sub = lax.broadcasted_iota(jnp.int32, (GROUP, LANES), 0)

    def wide(v):
        return jnp.concatenate([v] * (n // LANES), axis=1)

    groups = BLOCK // GROUP
    for block in range(first, last):
        base = block * BLOCK
        tile = [out_ref[pl.ds(base + g * GROUP, GROUP), :] for g in range(groups)]
        for g in range(groups):
            start = base + g * GROUP
            cols = [
                [
                    jnp.broadcast_to(tile[h][:, start + s : start + s + 1], (GROUP, LANES))
                    for h in range(g, groups)
                ]
                for s in range(GROUP)
            ]
            for s in range(GROUP):
                col = start + s
                scale = lax.rsqrt(jnp.broadcast_to(cols[s][0][s : s + 1, :], (GROUP, LANES)))
                factor = [c * scale for c in cols[s]]
                factor[0] = jnp.where(sub > s, factor[0], 0.0)
                pivot = jnp.broadcast_to(tile[g][s : s + 1, :], (GROUP, n)) * wide(scale)
                pivot = jnp.where(lane == col, wide(scale), pivot)
                for later in range(s + 1, GROUP):
                    entry = jnp.broadcast_to(cols[later][0][s : s + 1, :], (GROUP, LANES)) * scale
                    cols[later] = [c - f * entry for c, f in zip(cols[later], factor)]
                for h in range(g, groups):
                    if h == g:
                        kept = jnp.where((lane == col) & (wide(sub) > s), 0.0, tile[h])
                        new = kept - wide(factor[0]) * pivot
                        tile[h] = jnp.where(wide(sub) == s, pivot, new)
                    else:
                        kept = jnp.where(lane == col, 0.0, tile[h])
                        tile[h] = kept - wide(factor[h - g]) * pivot
        for g in range(groups):
            out_ref[pl.ds(base + g * GROUP, GROUP), :] = tile[g]
        rest = base + BLOCK
        if rest < n:
            rows = jnp.concatenate(tile, axis=0)
            lane_b = lax.broadcasted_iota(jnp.int32, (BLOCK, n), 1)
            row_b = lax.broadcasted_iota(jnp.int32, (BLOCK, n), 0) + base
            lower = jnp.where((lane_b > row_b) & (lane_b < rest), 0.0, rows)
            ah, am, al = split3(rows)
            bh, bm, bl = split3(lower)
            first = jnp.concatenate([ah, ah, ah, am, am, al], axis=0)
            second = jnp.concatenate([bh, bm, bl, bh, bm, bh], axis=0)
            change = lax.dot_general(
                first, second, (((0,), (0,)), ((), ())), preferred_element_type=F32
            )
            lane_r = lax.broadcasted_iota(jnp.int32, (n - rest, n), 1)
            old = out_ref[pl.ds(rest, n - rest), :]
            old = jnp.where((lane_r >= base) & (lane_r < rest), 0.0, old)
            out_ref[pl.ds(rest, n - rest), :] = old - change[rest:, :]
    if last * BLOCK == n:
        lane_n = lax.broadcasted_iota(jnp.int32, (n, n), 1)
        row_n = lax.broadcasted_iota(jnp.int32, (n, n), 0)
        out_ref[...] = jnp.where(row_n >= lane_n, out_ref[...], 0.0)


def dot(a, b, contract, precision=None):
    return lax.dot_general(
        a, b, (contract, ((), ())), precision=precision, preferred_element_type=F32
    )


NN = ((1,), (0,))
NT = ((1,), (1,))
TN = ((0,), (0,))


def struct(shape, dtype=F32):
    return jax.ShapeDtypeStruct(shape, dtype)


def kernel_call(kernel, out, flops, *args, grid=(), in_specs=None, out_specs=None, scratch=(), vmem=VMEM, prefetch=0):
    whole = pl.BlockSpec(memory_space=pltpu.VMEM)
    many = isinstance(out, (tuple, list))
    if in_specs is None:
        in_specs = [None] * len(args)
    specs = []
    for i, (spec, arg) in enumerate(zip(in_specs, args)):
        if i < prefetch:
            continue
        if spec is None:
            spec = pl.BlockSpec(memory_space=pltpu.SMEM) if arg.dtype == jnp.int32 else whole
        specs.append(spec)
    if out_specs is None:
        out_specs = type(out)([whole] * len(out)) if many else whole
    moved = sum(a.size * a.dtype.itemsize for a in list(args) + list(out if many else [out]))
    return pl.pallas_call(
        kernel,
        out_shape=out,
        grid_spec=pltpu.PrefetchScalarGridSpec(
            num_scalar_prefetch=prefetch,
            grid=grid,
            in_specs=specs,
            out_specs=out_specs,
            scratch_shapes=list(scratch),
        ),
        cost_estimate=pl.CostEstimate(flops=flops, bytes_accessed=moved, transcendentals=0),
        compiler_params=pltpu.CompilerParams(vmem_limit_bytes=vmem * 1024 * 1024),
    )(*args)


def split2(value):
    high = value.astype(BF16)
    return high, (value - high.astype(F32)).astype(BF16)


def rows_at(index, rows):
    return pl.ds(pl.multiple_of(index * rows, rows), rows)


def chol_inverse(state, first, last):
    kernel = functools.partial(chol_inverse_kernel, first, last)
    return kernel_call(kernel, struct(state.shape), 2_000_000_000, state)


def tied(values, *others):
    return lax.optimization_barrier((values, others))[0]


def fill_pair(pair_ref, pieces, place, scale=1.0):
    rows, rank = pieces[0].shape
    for m, piece in enumerate(pieces):
        high, low = split2(piece[...] * scale if scale != 1.0 else piece[...])
        at = rows_at(place(m), rows)
        pair_ref[at, :rank] = high
        pair_ref[at, rank:] = low


def basis_kernel(first, count, where_ref, grads_ref, *refs):
    pieces, (pair_ref, out_ref) = refs[: 2 * count], refs[-2:]
    rows, rank = pieces[0].shape
    fill_pair(pair_ref, pieces, lambda m: (m // 2) * 2 + ((where_ref[0] ^ m) & 1))
    total = refs[2 * count][...] if first else None
    for m in range(count):
        block = (where_ref[0] >> 1) ^ (first + m)
        columns = pl.ds(pl.multiple_of(block * (2 * rows), 2 * rows), 2 * rows)
        both = dot(grads_ref[:, columns], pair_ref[m * 2 * rows : (m + 1) * 2 * rows, :], NN)
        term = both[:, :rank] + both[:, rank:]
        total = term if total is None else total + term
    out_ref[...] = total


def momentum_kernel(first, where_ref, momentum_ref, pair_ref, *refs):
    out_ref = refs[-1]
    rank = out_ref.shape[1]
    high, low = split2(momentum_ref[...])
    both = dot(high, pair_ref[...], NN)
    term = 0.95 * (both[:, :rank] + both[:, rank:] + dot(low, pair_ref[:, :rank], NN))

    if first == 0:
        out_ref[...] = term
        return

    @pl.when(pl.program_id(1) == 0)
    def _():
        out_ref[...] = refs[0][...] + term

    @pl.when(pl.program_id(1) != 0)
    def _():
        out_ref[...] = out_ref[...] + term


SPLIT = 2


def chunk_of(q, index):
    return (q ^ (index // SPLIT)) * SPLIT + index % SPLIT


def left_kernel(count, scale, where_ref, acts_ref, base_ref, *refs):
    pieces, outs, (pair_ref, full_ref) = refs[:count], refs[count:-2], refs[-2:]
    rank = pieces[0].shape[1]
    fill_pair(pair_ref, pieces, lambda m: where_ref[0] ^ m)
    both = dot(acts_ref[...], pair_ref[...], TN)
    full_ref[...] = scale * (base_ref[...] + (both[:, :rank] + both[:, rank:]))
    for m, out_ref in enumerate(outs):
        out_ref[...] = full_ref[rows_at(chunk_of(where_ref[1], m), out_ref.shape[0]), :]


def buffer_kernel(count, where_ref, acts_ref, momentum_ref, *refs):
    pieces, (high_ref, low_ref) = refs[:count], refs[count:]
    rows, columns = pieces[0].shape
    step = 512
    lhs = [acts_ref[rows_at(where_ref[0] ^ m, rows), :] for m in range(count)]
    for start in range(0, columns, step):
        at = slice(start, start + step)
        total = 0.95 * momentum_ref[:, at]
        for m in range(count):
            total = total + dot(lhs[m], pieces[m][:, at], TN)
        high_ref[:, at], low_ref[:, at] = split2(total)


def gram_kernel(*refs):
    pieces, out_ref = refs[:-1], refs[-1]
    total = None
    for piece in pieces:
        value = piece[...]
        term = dot(value, value, TN, HIGHEST)
        total = term if total is None else total + term
    out_ref[...] = total


def share_kernel(quad, scale, where_ref, high_ref, low_ref, *refs):
    pieces, (out_ref, pair_ref) = refs[:-2], refs[-2:]
    rank = pieces[0].shape[1]

    @pl.when((pl.program_id(0) == 0) & (pl.program_id(1) == 0))
    def _():
        fill_pair(pair_ref, pieces, lambda m: chunk_of(where_ref[1], m), scale)

    both = dot(pair_ref[...], high_ref[...], TN)
    total = both[:rank] + both[rank:] + dot(pair_ref[:, :rank], low_ref[...], TN)
    total = total.T
    chunk = total.shape[0] // quad
    for c in range(quad):
        out_ref[0, 0, rows_at(where_ref[1] ^ c, chunk), :] = total[c * chunk : (c + 1) * chunk]


EXTRA = 16


def with_squares(ref, start, squares):
    ref[start : start + EXTRA, :] = jnp.zeros((EXTRA, ref.shape[1]), BF16)
    for i, part in enumerate(split3(squares)):
        ref[start + i : start + i + 1, :] = part


def squares_of(ref, start):
    part = ref[start : start + EXTRA, :].astype(F32)
    return part[0:1] + part[1:2] + part[2:3]


def right_kernel(part_ref, inverse_ref, right_ref, narrow_ref):
    right = dot(part_ref[...], inverse_ref[...], NT, HIGHEST)
    rows = right.shape[0]
    right_ref[...] = right
    narrow_ref[:rows, :] = right.astype(BF16)
    with_squares(narrow_ref, rows, jnp.sum(right * right, axis=0, keepdims=True))


def ortho_kernel(where_ref, inverse_ref, *refs):
    pieces, (out_ref, narrow_ref) = refs[:-2], refs[-2:]
    rows = pieces[0].shape[0]
    for m, piece in enumerate(pieces):
        at = rows_at(chunk_of(where_ref[1], m), rows)
        value = dot(piece[...], inverse_ref[...], NT, HIGHEST)
        out_ref[at, :] = value
        narrow_ref[at, :] = value.astype(BF16)


def collect_kernel(xs, quad, where_ref, *refs):
    exact, narrow = refs[:quad], refs[quad : xs * quad]
    own_ref, side_ref = refs[-2:]
    rows = exact[0].shape[0]
    squares = None
    for m in range(quad):
        value = exact[m][...]
        own_ref[rows_at(where_ref[1] ^ m, rows), :] = value
        terms = [jnp.sum(value * value, axis=0, keepdims=True)]
        for x in range(xs):
            at = rows_at(x * quad + (where_ref[1] ^ m), rows)
            if x == 0:
                side_ref[at, :] = value.astype(BF16)
            else:
                piece = narrow[(x - 1) * quad + m]
                side_ref[at, :] = piece[:rows, :]
                terms.append(squares_of(piece, rows))
        for term in terms:
            squares = term if squares is None else squares + term
    with_squares(side_ref, xs * quad * rows, squares)


def update_kernel(xs, where_ref, high_ref, low_ref, ortho_ref, side_ref, other_ref, own_ref, out_ref, new_ref, full_ref):
    rows = own_ref.shape[0]

    @pl.when(pl.program_id(0) == 0)
    def _():
        for x in range(xs):
            at = slice(x * rows, (x + 1) * rows)
            full_ref[rows_at(where_ref[0] ^ (2 * x), rows), :] = side_ref[at, :]
            full_ref[rows_at(where_ref[0] ^ (2 * x + 1), rows), :] = other_ref[at, :]
        squares = squares_of(side_ref, xs * rows) + squares_of(other_ref, xs * rows)
        new_ref[...] = own_ref[...] * lax.rsqrt(squares + 1e-06)

    step = 512
    for start in range(0, out_ref.shape[1], step):
        at = slice(start, start + step)
        change = dot(ortho_ref[...], full_ref[at, :], NT)
        value = high_ref[:, at].astype(F32) + low_ref[:, at].astype(F32)
        out_ref[:, at] = value - 0.05 * change


class Exchange:
    def __init__(self, replicas, parts):
        self.replicas, self.parts = replicas, parts
        self.quad = min(4, replicas)
        self.xs = parts // 2
        self.higher = []
        bit = self.quad
        while bit < replicas:
            self.higher.append(bit | (bit >> 1))
            bit *= 2
        d, self.t = lax.axis_index("dp"), lax.axis_index("tensor")
        bits, k, above = [], replicas.bit_length() - 2, 0
        while k >= 0:
            own = (d >> k) & 1
            if k >= 1 and (1 << (k + 1)) < replicas:
                own = own ^ above
            bits.append((k, own))
            above = own
            k -= 1
        self.q = sum(own << k for k, own in bits if (1 << k) < self.quad)
        self.x, self.core = self.t // 2, self.t % 2

    def swap(self, value, dp=0, tensor=0):
        n, m = self.parts, self.replicas
        if dp == 0:
            return lax.ppermute(value, "tensor", [(i, i ^ tensor) for i in range(n)])
        if tensor == 0:
            return lax.ppermute(value, "dp", [(i, i ^ dp) for i in range(m)])
        pairs = [((i // n), i % n) for i in range(m * n)]
        perm = [(d * n + t, (d ^ dp) * n + (t ^ tensor)) for d, t in pairs]
        return lax.ppermute(value, ("dp", "tensor"), perm)

    def gather_tensor(self, value):
        pieces = {0: value, 1: self.swap(value, tensor=1)}
        for m in range(2, self.parts, 2):
            pieces[m] = self.swap(value, tensor=m)
            pieces[m + 1] = self.swap(pieces[m], tensor=1)
        return [pieces[m] for m in range(self.parts)]


def step(acts, out_grad, momentum, q_basis):
    replicas, parts = lax.axis_size("dp"), lax.axis_size("tensor")
    ex = Exchange(replicas, parts)
    rows, columns = momentum.shape
    tokens = acts.shape[0]
    rank = q_basis.shape[1]
    tile = 256 if rows % 256 == 0 else 128
    large = rows // 2
    steps = rows // tile
    where = jnp.stack([ex.t, ex.q]).astype(jnp.int32)
    wide_spec = pl.BlockSpec((tile, columns), lambda i: (i, 0))
    rank_spec = pl.BlockSpec((tile, rank), lambda i: (i, 0))
    acts_spec = pl.BlockSpec((tokens, tile), lambda i: (0, i))

    xs, local = ex.xs, columns // parts
    half = 2 * local
    where_x = jnp.stack([ex.x, ex.q]).astype(jnp.int32)
    near = [q_basis, ex.swap(q_basis, tensor=1)]
    across = [ex.swap(q_basis, tensor=m) for m in range(2, parts, 2)]

    def basis(first, pieces, *more):
        count = len(pieces) // 2
        return kernel_call(
            functools.partial(basis_kernel, first, count),
            (struct((count * half, 2 * rank), BF16), struct((out_grad.shape[0], rank))),
            4 * out_grad.shape[0] * count * half * rank, where, out_grad, *pieces, *more,
        )

    near_pair, near_grad = basis(0, near)
    base = kernel_call(
        functools.partial(momentum_kernel, 0), struct((rows, rank)),
        6 * rows * half * rank, where_x, momentum, near_pair, grid=(2,), prefetch=1,
        in_specs=[None, pl.BlockSpec((large, half), lambda i, w: (i, w[0])), None],
        out_specs=pl.BlockSpec((large, rank), lambda i, w: (i, 0)), vmem=LARGE,
    )
    far = []
    for piece in tied(across, base):
        far += [piece, ex.swap(piece, tensor=1)]
    pair, grad_q = basis(1, far, near_grad)
    base = kernel_call(
        functools.partial(momentum_kernel, 1), struct((rows, rank)),
        6 * rows * (columns - half) * rank, where_x, momentum, pair, base,
        grid=(2, xs - 1), prefetch=1,
        in_specs=[
            None,
            pl.BlockSpec((large, half), lambda i, j, w: (i, w[0] ^ (j + 1))),
            pl.BlockSpec((half, 2 * rank), lambda i, j, w: (j, 0)),
            pl.BlockSpec((large, rank), lambda i, j, w: (i, 0)),
        ],
        out_specs=pl.BlockSpec((large, rank), lambda i, j, w: (i, 0)), vmem=LARGE,
    )
    near_q = ex.swap(grad_q, tensor=1)
    far_q = tied([ex.swap(grad_q, tensor=m) for m in range(2, parts, 2)], base)
    grads_q = [grad_q, near_q]
    for value in far_q:
        grads_q += [value, ex.swap(value, tensor=1)]
    left = kernel_call(
        functools.partial(left_kernel, parts, 1.0 / replicas),
        [struct((rows // (SPLIT * ex.quad), rank))] * (SPLIT * ex.quad),
        4 * rows * tokens * rank, where, acts, base, *grads_q,
        scratch=[pltpu.VMEM((tokens, 2 * rank), BF16), pltpu.VMEM((rows, rank), F32)], vmem=LEFT,
    )

    quad = range(1, ex.quad)
    received = []
    for h in range(SPLIT):
        received.append([ex.swap(left[m * SPLIT + h], dp=m) for m in quad])
    grads = {0: out_grad, 1: ex.swap(out_grad, tensor=1)}
    sums = []
    for h in range(SPLIT):
        total = left[h]
        for piece in tied(received[h], sums):
            total = total + piece
        sums.append(total)
    held = tied(out_grad, grads_q[1:])
    for m in range(2, parts, 2):
        grads[m] = ex.swap(held, tensor=m)
    for mask in ex.higher:
        others = [ex.swap(value, dp=mask) for value in sums]
        added = []
        for value, other in zip(sums, others):
            added.append(value + tied(other, added))
        sums = added
    for m in range(2, parts, 2):
        grads[m] = tied(grads[m], sums)
        grads[m + 1] = ex.swap(grads[m], tensor=1)
    lefts = list(sums)
    for m in quad:
        for h in range(SPLIT):
            lefts.append(ex.swap(sums[h], dp=m))
    grads = [grads[m] for m in range(parts)]

    high, low = kernel_call(
        functools.partial(buffer_kernel, parts),
        (struct((rows, columns), BF16), struct((rows, columns), BF16)),
        2 * rows * tokens * columns, where, acts, momentum, *grads, grid=(steps,),
        in_specs=[None, acts_spec, wide_spec] + [None] * parts, out_specs=(wide_spec, wide_spec), vmem=BUFFER,
    )

    lefts[SPLIT:] = tied(lefts[SPLIT:], high)
    gram = kernel_call(gram_kernel, struct((rank, rank)), 12 * rows * rank * rank, *lefts)
    lefts_b = tied(lefts, gram)
    near_gram = ex.swap(gram, tensor=1)
    blocks = rank // BLOCK
    count = xs * ex.quad

    def shares(other, first, number):
        core = 1 - ex.core if other else ex.core
        at = jnp.stack([ex.x * 2 + core, ex.q, core]).astype(jnp.int32)
        spec = pl.BlockSpec((rows, local), lambda i, j, w: (0, w[0] ^ (2 * (i + first))))
        return kernel_call(
            functools.partial(share_kernel, ex.quad, 1.0 / replicas),
            struct((number, 1, local, rank)), 6 * rows * number * local * rank,
            at, high, low, *lefts_b, grid=(number, 1), prefetch=1,
            in_specs=[None, spec, spec] + [None] * len(lefts_b),
            out_specs=pl.BlockSpec((1, 1, local, rank), lambda i, j, w: (i, 0, 0, 0)),
            scratch=[pltpu.VMEM((rows, 2 * rank), BF16)], vmem=VMEM,
        ).reshape(number * ex.quad, local // ex.quad, rank)

    send = shares(True, 0, xs)
    got = ex.swap(send, tensor=1)
    gram = gram + tied(near_gram, send)
    grams = [ex.swap(gram, tensor=m) for m in range(2, parts, 2)]
    keep = shares(False, 0, xs)
    share = keep + got
    part = share[0]
    pieces = [
        ex.swap(share[m], dp=m % ex.quad, tensor=2 * (m // ex.quad)) for m in range(1, count)
    ]
    total = gram
    for piece in tied(grams, pieces[-1]):
        total = total + piece
    state = chol_inverse(total, 0, blocks // 2)
    for piece in tied(pieces, state):
        part = part + piece
    inverse = chol_inverse(tied(state, part), blocks // 2, blocks)
    for mask in ex.higher:
        part = part + tied(ex.swap(part, dp=mask), inverse)

    right, narrow = kernel_call(
        right_kernel, (struct(part.shape), struct((part.shape[0] + EXTRA, rank), BF16)),
        12 * part.shape[0] * rank * rank, part, inverse,
    )
    exact = [right] + [ex.swap(right, dp=m) for m in quad]
    across = [
        ex.swap(narrow, dp=m % ex.quad, tensor=2 * (m // ex.quad)) for m in range(ex.quad, count)
    ]
    ortho, narrow = kernel_call(
        ortho_kernel,
        (struct((rows, rank)), struct((rows, rank), BF16)),
        12 * rows * rank * rank, tied(where, right), inverse, *lefts,
    )
    exact[1:], across = tied((exact[1:], across), ortho)
    own, side = kernel_call(
        functools.partial(collect_kernel, xs, ex.quad),
        (struct((local, rank)), struct((xs * local + EXTRA, rank), BF16)),
        2 * local * rank, where, *exact, *across,
    )
    other = ex.swap(side, tensor=1)
    new_momentum, new_q = kernel_call(
        functools.partial(update_kernel, xs),
        (struct((rows, columns)), struct((local, rank))),
        2 * rows * columns * rank, where, high, low, narrow, side, other, own, grid=(steps,),
        in_specs=[None, wide_spec, wide_spec, rank_spec, None, None, None],
        out_specs=(wide_spec, pl.BlockSpec((local, rank), lambda i: (0, 0))),
        scratch=[pltpu.VMEM((columns, rank), BF16)], vmem=VMEM,
    )
    return (new_momentum, ortho, new_q)


def solution(mesh):
    in_specs = (
        P("dp", "tensor"),
        P(("dp", "tensor"), None),
        P(("dp", "tensor"), None),
        P("tensor", None),
    )
    out_specs = (P(("dp", "tensor"), None), P("tensor", None), P("tensor", None))
    return jax.shard_map(step, mesh=mesh, in_specs=in_specs, out_specs=out_specs, check_vma=False)
```
